8 devices in a mesh: rep: 1 (over z), dp: 8 (over x, y, core).
Axes of the slice: x: 2, y: 2, z: 1, core: 2. Of those that a mesh axis runs over, the one named last changes fastest.
Arguments:
- x: bfloat16 [8, 2048, 1024], P(('rep', 'dp'))
- dy: bfloat16 [8, 2048, 1024], P(('rep', 'dp'))
- w_gate: bfloat16 [2, 1024, 3200], P(None, 'dp')
- w_up: bfloat16 [2, 1024, 3200], P(None, 'dp')
- w_down: bfloat16 [2, 3200, 1024], P(None, 'dp')
- m_w_gate: float32 [2, 1024, 3200], P(None, 'dp')
- m_w_up: float32 [2, 1024, 3200], P(None, 'dp')
- m_w_down: float32 [2, 3200, 1024], P(None, 'dp')
- v_w_gate: float32 [2, 1024, 3200], P(None, 'dp')
- v_w_up: float32 [2, 1024, 3200], P(None, 'dp')
- v_w_down: float32 [2, 3200, 1024], P(None, 'dp')
Outputs:
- output 1: bfloat16 [2, 1024, 3200], P('rep', 'dp')
- output 2: bfloat16 [2, 1024, 3200], P('rep', 'dp')
- output 3: bfloat16 [2, 3200, 1024], P('rep', 'dp')
- output 4: float32 [2, 1024, 3200], P('rep', 'dp')
- output 5: float32 [2, 1024, 3200], P('rep', 'dp')
- output 6: float32 [2, 3200, 1024], P('rep', 'dp')
- output 7: float32 [2, 1024, 3200], P('rep', 'dp')
- output 8: float32 [2, 1024, 3200], P('rep', 'dp')
- output 9: float32 [2, 3200, 1024], P('rep', 'dp')
All inputs are finite; a program needn't handle non-finite values.
Results may differ from the reference program's by a relative error of at most 0.022.
Values are sent between devices in bfloat16 or wider.
A program may use at most 2 GiB of HBM per device.

```python
import jax
import jax.numpy as jnp
from jax import lax

SEQUENCES = 8
TOKENS = 2048
D = 1024
FF = 3200
LAYERS = 2
NAMES = ("w_gate", "w_up", "w_down")
SHAPES = {"w_gate": (LAYERS, D, FF), "w_up": (LAYERS, D, FF), "w_down": (LAYERS, FF, D)}


def bump(key, n, height):
    away = (jnp.arange(n, dtype=jnp.int32) - jax.random.randint(key, (), 0, n, jnp.int32)) % n
    return jnp.where(away < n // 8, height, 1.0)


def together(key, own, strength):
    shared = jax.random.normal(key, own.shape[1:], jnp.float32)
    return (own + strength * shared) * lax.rsqrt(1 + strength * strength)


def setup_inputs(seed: int = 0, part: int = 0) -> dict:
    kx, kdy, ka, kb, kz, kf, kh, kl, *keys = jax.random.split(jax.random.key(seed), 8 + 3 * len(NAMES))
    kx, kdy, ka, kb = (jax.random.fold_in(k, part) for k in (kx, kdy, ka, kb))
    kw, km, kv = (keys[i::3] for i in range(3))
    shape = (SEQUENCES, TOKENS, D)
    much_x, much_dy = jax.random.uniform(kz, (2,), jnp.float32, 0.0, 1.0)
    loud = 2.0 ** jax.random.uniform(jax.random.fold_in(kz, 1), (), jnp.float32, -1.0, 2.0)
    layers = 2.0 ** jax.random.uniform(kl, (LAYERS, 1, 1), jnp.float32, -1.0, 1.0)
    x = together(ka, jax.random.normal(kx, shape, jnp.float32), much_x) * bump(kf, D, 4.0)
    dy = together(kb, jax.random.normal(kdy, shape, jnp.float32), much_dy)
    drawn = {"x": x.astype(jnp.bfloat16), "dy": (loud * dy * (SEQUENCES * TOKENS) ** -0.5).astype(jnp.bfloat16)}
    for key, name in zip(kw, NAMES, strict=True):
        w = jax.random.normal(key, SHAPES[name], jnp.float32) * SHAPES[name][1] ** -0.5
        drawn[name] = (w * {"w_gate": 1.0, "w_up": bump(kh, FF, 4.0), "w_down": layers}[name]).astype(jnp.bfloat16)
    for key, name in zip(km, NAMES, strict=True):
        drawn[f"m_{name}"] = 0.1 * jax.random.normal(key, SHAPES[name], jnp.float32)
    for key, name in zip(kv, NAMES, strict=True):
        drawn[f"v_{name}"] = jax.random.uniform(key, SHAPES[name], jnp.float32, 0.005, 0.015)
    return drawn


def matmul(a, w):
    return jnp.dot(a, w, preferred_element_type=jnp.float32).astype(jnp.bfloat16)


def normed(h):
    wide = h.astype(jnp.float32)
    scale = lax.rsqrt(jnp.mean(wide**2, -1, keepdims=True) + 1e-6)
    return (wide * scale).astype(jnp.bfloat16)


def layer(h, w):
    a = normed(h)
    gate = jnp.dot(a, w["w_gate"], preferred_element_type=jnp.float32)
    up = jnp.dot(a, w["w_up"], preferred_element_type=jnp.float32)
    return h + matmul((jax.nn.silu(gate) * up).astype(jnp.bfloat16), w["w_down"])


def adamw(w, m, v, g):
    m = 0.9 * m + 0.1 * g
    v = 0.95 * v + 0.05 * g * g
    step = m * lax.rsqrt(v + 1e-8) + 0.1 * w
    return (w - 0.02 * step).astype(jnp.bfloat16), m, v


def clipped(gradients, sum_of_squares, count):
    factor = jnp.minimum(1.0, 0.5 * lax.rsqrt(sum_of_squares / count + 1e-30))
    return [g * factor for g in gradients]


def stack(weights, h):
    return lax.scan(lambda h, w: (layer(h, w), None), h, weights)[0]


def reference(x, dy, w_gate, w_up, w_down, m_w_gate, m_w_up, m_w_down, v_w_gate, v_w_up, v_w_down):
    weights = dict(zip(NAMES, (w_gate, w_up, w_down), strict=True))

    def take(so_far, sequence):
        h, by_y = sequence
        _, back = jax.vjp(lambda w: stack(w, h), weights)
        return jax.tree.map(lambda total, term: total + term.astype(jnp.float32), so_far, back(by_y)[0]), None

    none_yet = {name: jnp.zeros(w.shape, jnp.float32) for name, w in weights.items()}
    by_weights, _ = lax.scan(take, none_yet, (x, dy))
    gradients = [by_weights[name].astype(jnp.bfloat16).astype(jnp.float32) for name in NAMES]
    gradients = clipped(gradients, sum(jnp.sum(g * g) for g in gradients), sum(g.size for g in gradients))
    new = [
        adamw(w.astype(jnp.float32), m, v, g)
        for w, m, v, g in zip((w_gate, w_up, w_down), (m_w_gate, m_w_up, m_w_down), (v_w_gate, v_w_up, v_w_down), gradients, strict=True)
    ]
    return tuple(one[which] for which in range(3) for one in new)
```

```python
import functools

import jax
import jax.numpy as jnp
from jax import lax
from jax.experimental import pallas as pl
from jax.experimental.pallas import tpu as pltpu
from jax.sharding import PartitionSpec as P


F32, BF16 = jnp.float32, jnp.bfloat16
T, D, FF = 2048, 1024, 3200
RG, RD = D // 8, FF // 8
CUT = 208
TILE = 256
ANY = pl.BlockSpec(memory_space=pl.ANY)
NN, NT, TN = (((1,), (0,)), ((), ())), (((1,), (1,)), ((), ())), (((0,), (0,)), ((), ()))


def dot(a, b, how=NN):
    return lax.dot_general(a, b, how, preferred_element_type=F32)


def send(x, mask):
    return lax.ppermute(x, "dp", [(i, i ^ mask) for i in range(8)])


def place(mask):
    me = lax.axis_index("dp")
    bits = [me // 4, (me // 2) % 2, me % 2]
    flip = [(mask >> 2) & 1, (mask >> 1) & 1, mask & 1]
    x, y, c = [1 - b if f else b for b, f in zip(bits, flip, strict=True)]
    return x * 4 + y * 2 + c


def gather(shard, cut):
    x, y = send(shard, 4), send(shard, 2)
    da, db = send(x[:cut], 2), send(y[cut:], 4)
    mine = [(0, 0, shard), (4, 0, x), (2, 0, y), (6, 0, da), (6, cut, db)]
    return mine + [(m ^ 1, r, send(a, 1)) for m, r, a in mine]


def gate_up_copies(pieces, refs, wg, wu, sem):
    out = []
    for (mask, first, _), ref in zip(pieces, refs, strict=True):
        rows = pl.ds(pl.multiple_of(place(mask) * RG, RG), RG)
        if ref.shape[0] == 2 * RG:
            out += [(ref.at[:RG], wg.at[rows]), (ref.at[RG:], wu.at[rows])]
        else:
            out.append((ref, (wu if first else wg).at[rows]))
    return [pltpu.make_async_copy(s, d, sem.at[k]) for k, (s, d) in enumerate(out)]


def down_copies(pieces, refs, wd, sem):
    out = []
    for (mask, first, _), ref in zip(pieces, refs, strict=True):
        rows = pl.ds(pl.multiple_of(place(mask) * RD + first, 16), ref.shape[0])
        out.append((ref, wd.at[rows]))
    return [pltpu.make_async_copy(s, d, sem.at[k]) for k, (s, d) in enumerate(out)]


def load(copies):
    @pl.when(pl.program_id(0) == 0)
    def _():
        for c in copies:
            c.start()
        for c in copies:
            c.wait()


def rows(width):
    return pl.BlockSpec((TILE, width), lambda i: (i, 0))


def call(body, name, flops, grid, in_specs, out_specs, out_shape, scratch):
    return pl.pallas_call(
        body,
        name=name,
        grid=grid,
        in_specs=in_specs,
        out_specs=out_specs,
        out_shape=out_shape,
        scratch_shapes=scratch,
        cost_estimate=pl.CostEstimate(flops=flops, bytes_accessed=30_000_000, transcendentals=0),
        compiler_params=pltpu.CompilerParams(vmem_limit_bytes=62 * 2**20, dimension_semantics=("arbitrary",) * len(grid)),
    )


def shape(*s, dtype=BF16):
    return jax.ShapeDtypeStruct(s, dtype)


MM = 2 * T * D * FF
WG = pltpu.VMEM((D, FF), BF16)
WD = pltpu.VMEM((FF, D), BF16)
SEM = pltpu.SemaphoreType.DMA((16,))


def scale_of(wide):
    return lax.rsqrt(jnp.mean(wide**2, -1, keepdims=True) + 1e-6)


def norm(h):
    wide = h.astype(F32)
    return (wide * scale_of(wide)).astype(BF16)


def forward_gate_up(x, pieces):
    def body(x_ref, *refs):
        n = len(pieces)
        a_out, hid_out, g_out, u_out, wg, wu, sem = refs[n:]
        load(gate_up_copies(pieces, refs[:n], wg, wu, sem))
        a = norm(x_ref[...])
        a_out[...] = a
        g = dot(a, wg[...])
        u = dot(a, wu[...])
        g_out[...] = g
        u_out[...] = u
        hid_out[...] = (g * jax.nn.sigmoid(g) * u).astype(BF16)

    return call(
        body, "fwd_gu", 2 * MM, (T // TILE,), [rows(D)] + [ANY] * len(pieces), [rows(D), rows(FF), rows(FF), rows(FF)],
        [shape(T, D), shape(T, FF), shape(T, FF, dtype=F32), shape(T, FF, dtype=F32)], [WG, WG, SEM],
    )(x, *[a for _, _, a in pieces])


def forward_down(hid, x, pieces):
    def body(hid_ref, x_ref, *refs):
        n = len(pieces)
        h_out, a_out, wd, sem = refs[n:]
        load(down_copies(pieces, refs[:n], wd, sem))
        h = x_ref[...] + dot(hid_ref[...], wd[...]).astype(BF16)
        h_out[...] = h
        a_out[...] = norm(h)

    return call(
        body, "fwd_down", MM, (T // TILE,), [rows(FF), rows(D)] + [ANY] * len(pieces), [rows(D), rows(D)],
        [shape(T, D), shape(T, D)], [WD, SEM],
    )(hid, x, *[a for _, _, a in pieces])


def back_down(by_h, pieces):
    def body(by_ref, *refs):
        n = len(pieces)
        out, wd, sem = refs[n:]
        load(down_copies(pieces, refs[:n], wd, sem))
        out[...] = dot(by_ref[...], wd[...], NT).astype(BF16)

    return call(
        body, "bwd_down", MM, (T // TILE,), [rows(D)] + [ANY] * len(pieces), rows(FF), shape(T, FF), [WD, SEM],
    )(by_h, *[a for _, _, a in pieces])


def gated(g, u, by_hid):
    sig = jax.nn.sigmoid(g)
    silu = g * sig
    return silu * u, by_hid * u * (sig * (1.0 + g * (1.0 - sig))), by_hid * silu


def last_gate_up(a, by_hid, pieces):
    def body(a_ref, by_ref, *refs):
        n = len(pieces)
        hid_out, by_out, wg, wu, sem = refs[n:]
        load(gate_up_copies(pieces, refs[:n], wg, wu, sem))
        g = dot(a_ref[...], wg[...])
        u = dot(a_ref[...], wu[...])
        hid, dg, du = gated(g, u, by_ref[...].astype(F32))
        hid_out[...] = hid.astype(BF16)
        by_out[0] = dg.astype(BF16)
        by_out[1] = du.astype(BF16)

    return call(
        body, "last_gu", 2 * MM, (T // TILE,), [rows(D), rows(FF)] + [ANY] * len(pieces),
        [rows(FF), pl.BlockSpec((2, TILE, FF), lambda i: (0, i, 0))], [shape(T, FF), shape(2, T, FF)], [WG, WG, SEM],
    )(a, by_hid, *[a for _, _, a in pieces])


def back_gate_up(by_gu, h, by_y, pieces):
    def body(by_ref, h_ref, y_ref, *refs):
        n = len(pieces)
        out, wg, wu, sem = refs[n:]
        load(gate_up_copies(pieces, refs[:n], wg, wu, sem))
        da = dot(by_ref[0], wg[...], NT) + dot(by_ref[1], wu[...], NT)
        wide = h_ref[...].astype(F32)
        s = scale_of(wide)
        by_h = da * s - wide * (s * s * s * jnp.mean(da * wide, -1, keepdims=True))
        out[...] = (y_ref[...].astype(F32) + by_h).astype(BF16)

    return call(
        body, "bwd_gu", 2 * MM, (T // TILE,), [pl.BlockSpec((2, TILE, FF), lambda i: (0, i, 0)), rows(D), rows(D)] + [ANY] * len(pieces),
        rows(D), shape(T, D), [WG, WG, SEM],
    )(by_gu, h, by_y, *[a for _, _, a in pieces])


def first_back_down(by_h, g, u, pieces):
    def body(by_ref, g_ref, u_ref, *refs):
        n = len(pieces)
        by_out, wd, sem = refs[n:]
        load(down_copies(pieces, refs[:n], wd, sem))
        by_hid = dot(by_ref[...], wd[...], NT).astype(BF16).astype(F32)
        _, dg, du = gated(g_ref[...], u_ref[...], by_hid)
        by_out[0] = dg.astype(BF16)
        by_out[1] = du.astype(BF16)

    return call(
        body, "first_bwd_down", MM, (T // TILE,), [rows(D), rows(FF), rows(FF)] + [ANY] * len(pieces),
        pl.BlockSpec((2, TILE, FF), lambda i: (0, i, 0)), shape(2, T, FF), [WD, SEM],
    )(by_h, g, u, *[a for _, _, a in pieces])


CHIPS = (0, 2, 4, 6)


def grad_down(hid, by_h):
    step = 640

    def body(hid_ref, by_ref, mine, other, total, sem):
        i = pl.program_id(0)
        total[pl.ds(pl.multiple_of(i * step, step), step), :] = dot(hid_ref[...], by_ref[...], TN).astype(BF16)

        @pl.when(i == FF // step - 1)
        def _():
            copies = []
            for k, mask in enumerate(CHIPS):
                for j, (out, m) in enumerate(((other, mask ^ 1), (mine, mask))):
                    part = total.at[pl.ds(pl.multiple_of(place(m) * RD, 16), RD)]
                    copies.append(pltpu.make_async_copy(part, out.at[k], sem.at[2 * k + j]))
            for c in copies:
                c.start()
            for c in copies:
                c.wait()

    return call(
        body, "grad_down", MM, (FF // step,), [pl.BlockSpec((T, step), lambda i: (0, i)), pl.BlockSpec((T, D), lambda i: (0, 0))],
        [ANY, ANY], [shape(4, RD, D), shape(4, RD, D)], [WD, pltpu.SemaphoreType.DMA((8,))],
    )(hid, by_h)


def grad_gate_up(a, by_gu):
    def chip(k):
        me = lax.axis_index("dp")
        x, y = me // 4, (me // 2) % 2
        fx, fy = k // 2, k % 2
        return (x + fx - 2 * x * fx) * 2 + (y + fy - 2 * y * fy)

    def body(a_ref, by_ref, mine, other, both):
        core = lax.axis_index("dp") % 2
        columns = pl.ds(pl.multiple_of(chip(pl.program_id(1)) * 2 * RG, 2 * RG), 2 * RG)
        both[...] = dot(a_ref[:, columns], by_ref[0], TN)
        mine[0, 0] = both[pl.ds(pl.multiple_of(core * RG, RG), RG), :].astype(BF16)
        other[0, 0] = both[pl.ds(pl.multiple_of((1 - core) * RG, RG), RG), :].astype(BF16)

    spec = pl.BlockSpec((1, 1, RG, FF), lambda w, k: (k, w, 0, 0))
    return call(
        body, "grad_gu", 2 * MM, (2, 4), [pl.BlockSpec((T, D), lambda w, k: (0, 0)), pl.BlockSpec((1, T, FF), lambda w, k: (w, 0, 0))],
        [spec, spec], [shape(4, 2, RG, FF)] * 2, [pltpu.VMEM((2 * RG, FF), F32)],
    )(a, by_gu)


def scatter(mine, other, cut):
    here = [mine[k].astype(F32) for k in range(4)]
    far = send(other, 1)
    pair = [h + far[k].astype(F32) for k, h in enumerate(here)]
    a = send(pair[3][:cut].astype(BF16), 4)
    b = send(pair[3][cut:].astype(BF16), 2)
    to_y = jnp.concatenate([pair[1][:cut] + a.astype(F32), pair[1][cut:]]).astype(BF16)
    to_x = jnp.concatenate([pair[2][:cut], pair[2][cut:] + b.astype(F32)]).astype(BF16)
    return (pair[0] + send(to_y, 2).astype(F32) + send(to_x, 4).astype(F32)).astype(BF16)


def adamw(w, m, v, g):
    m = 0.9 * m + 0.1 * g
    v = 0.95 * v + 0.05 * g * g
    step = m * lax.rsqrt(v + 1e-8) + 0.1 * w
    return (w - 0.02 * step).astype(BF16), m, v


def solution(mesh):
    def step(x, dy, *arrays):
        weights, m, v = (arrays[i : i + 3] for i in (0, 3, 6))
        x, dy = x[0], dy[0]
        gu = [gather(jnp.concatenate([weights[0][n], weights[1][n]]), RG) for n in range(1)]
        wd = [gather(weights[2][n], CUT) for n in range(2)]
        gu.append(gather(jnp.concatenate([weights[0][1], weights[1][1]]), RG))

        a0, hid0, g0, u0 = forward_gate_up(x, gu[0])
        h1, a1 = forward_down(hid0, x, wd[0])
        by_hid1 = back_down(dy, wd[1])
        hid1, by_gu1 = last_gate_up(a1, by_hid1, gu[1])
        sum_d1 = scatter(*grad_down(hid1, dy), CUT)
        sum_gu1 = scatter(*grad_gate_up(a1, by_gu1), 1)
        by_h1 = back_gate_up(by_gu1, h1, dy, gu[1])
        sum_d0 = scatter(*grad_down(hid0, by_h1), CUT)
        by_gu0 = first_back_down(by_h1, g0, u0, wd[0])
        sum_gu0 = scatter(*grad_gate_up(a0, by_gu0), 1)

        gradients = [jnp.stack([sum_gu0[0], sum_gu1[0]]), jnp.stack([sum_gu0[1], sum_gu1[1]]), jnp.stack([sum_d0, sum_d1])]
        gradients = [g.astype(F32) for g in gradients]
        squares = sum(jnp.sum(g * g) for g in gradients).reshape(1, 1)
        for mask in (1, 2, 4):
            squares = squares + send(squares, mask)
        count = 8 * sum(g.size for g in gradients)
        factor = jnp.minimum(1.0, 0.5 * lax.rsqrt(squares[0, 0] / count + 1e-30))
        new = [adamw(w.astype(F32), m, v, g * factor) for w, m, v, g in zip(weights, m, v, gradients, strict=True)]
        return tuple(one[which] for which in range(3) for one in new)

    states, cut = P(("rep", "dp"), None, None), P(None, "dp", None)
    return jax.shard_map(
        step,
        mesh=mesh,
        in_specs=(states, states) + (cut,) * 9,
        out_specs=(P("rep", "dp", None),) * 9,
        check_vma=False,
    )
```
